32 devices in a mesh: gx: 2 (over y), gy: 4 (over z), gz: 4 (over x, core).
Axes of the slice: x: 2, y: 2, z: 4, core: 2. Of those that a mesh axis runs over, the one named last changes fastest.
Arguments:
- tokens: bfloat16 [512, 6144], P(('gx', 'gy'), 'gz'), may hold values from -6 to 6
- grad_out: bfloat16 [512, 6144], P(('gx', 'gy'), 'gz'), may hold values from -1.5 to 1.5
- w_in: bfloat16 [6144, 12288], P('gz', ('gy', 'gx')), may hold values from -0.078125 to 0.078125
- w_out: bfloat16 [12288, 6144], P(('gy', 'gx'), 'gz'), may hold values from -0.0546875 to 0.0546875
Outputs:
- mlp_out: bfloat16 [512, 6144], P(('gx', 'gy'), 'gz')
- tok_grad: bfloat16 [512, 6144], P(('gx', 'gy'), 'gz')
- win_grad: float32 [6144, 12288], P('gz', ('gy', 'gx'))
- wout_grad: float32 [12288, 6144], P(('gy', 'gx'), 'gz')
The draws below stay inside these ranges and needn't reach their ends.
All inputs are finite; a program needn't handle non-finite values.
Results may differ from the reference program's by a relative error of at most 0.01.
Values may be sent and summed in bfloat16 or wider, within the bound.
No kernel may reach another device: no remote copies, remote signals or barrier semaphores. Data moves between devices by JAX's collectives and lax.ppermute only.
A program may use at most 128 MiB of HBM per device.

```python
import math
import jax
import jax.numpy as jnp
from jax import lax

D = 6144
FF = 12288
ROWS = 256
TOKENS = 512
N_GX = 2


def shard_levels(own_key, dims, shards, least, high):
    factor_of, own = 1.0, jax.random.fold_in(own_key, 6)
    for position, parts in shards:
        draws = jnp.exp(jax.random.uniform(jax.random.fold_in(own, position), (parts,), jnp.float32, least / len(shards), high / len(shards)))
        factor_of = factor_of * jnp.repeat(draws, dims[position] // parts).reshape([-1 if axis == position else 1 for axis in range(len(dims))])
    return factor_of


def centred(own_key, dims, spread, bound, shards=(), held_as=jnp.bfloat16):
    array = spread * jax.random.normal(own_key, dims, jnp.float32)
    if shards:
        array = array * shard_levels(own_key, dims, shards, -0.22, 0.18)
    return jnp.clip(array, -bound, bound).astype(held_as)


def setup_inputs(seed: int = 0) -> dict:
    keys = jax.random.split(jax.random.key(seed), 5)
    tokens = centred(keys[0], (TOKENS, D), 1.0, 6.0, ((0, 8), (1, 4)))
    grad_out = centred(keys[1], (TOKENS, D), 0.25, 1.5, ((0, 8), (1, 4)))
    w_in = centred(keys[2], (D, FF), D ** -0.5, 0.078125, ((0, 4), (1, 8)))
    w_out = centred(keys[3], (FF, D), FF ** -0.5, 0.0546875, ((0, 8), (1, 4)))
    return {"tokens": tokens, "grad_out": grad_out, "w_in": w_in, "w_out": w_out}


def gelu_slope(values):
    cdf = 0.5 * (1.0 + jax.scipy.special.erf(values * 0.7071067811865476))
    density = jnp.exp(-0.5 * values * values) * 0.3989422804014327
    return cdf + values * density

def reference(tokens, grad_out, w_in, w_out):
    block_scale = 1.0 / math.sqrt(ROWS)
    pre = jnp.dot(tokens, w_in, preferred_element_type=jnp.float32)
    act = jax.nn.gelu(pre, approximate=False).astype(jnp.bfloat16)
    mlp_out = jnp.dot(act, w_out, preferred_element_type=jnp.float32).astype(jnp.bfloat16)
    d_act = jnp.dot(grad_out, w_out.T, preferred_element_type=jnp.float32)
    d_pre = (d_act * gelu_slope(pre)).astype(jnp.bfloat16)
    tok_grad = jnp.dot(d_pre, w_in.T, preferred_element_type=jnp.float32).astype(jnp.bfloat16)
    wout_grad = jnp.zeros((FF, D), jnp.float32)
    win_grad = jnp.zeros((D, FF), jnp.float32)
    for block in range(N_GX):
        lower = block * ROWS
        part_out = (jnp.dot(act[lower:lower + ROWS].T, grad_out[lower:lower + ROWS], preferred_element_type=jnp.float32) * block_scale).astype(jnp.bfloat16)
        part_in = (jnp.dot(tokens[lower:lower + ROWS].T, d_pre[lower:lower + ROWS], preferred_element_type=jnp.float32) * block_scale).astype(jnp.bfloat16)
        part_out = lax.optimization_barrier(part_out)
        part_in = lax.optimization_barrier(part_in)
        wout_grad = wout_grad + part_out.astype(jnp.float32)
        win_grad = win_grad + part_in.astype(jnp.float32)
    return (mlp_out, tok_grad, win_grad, wout_grad)
```

```python
import math

import jax
import jax.numpy as jnp
from jax import lax
from jax.sharding import PartitionSpec as P


def gelu_and_slope(values):
    cdf = 0.5 * (1.0 + lax.erf(values * 0.7071067811865476))
    density = jnp.exp(-0.5 * values * values) * 0.3989422804014327
    return values * cdf, cdf + values * density


def contract(left, right, left_dim, right_dim):
    return lax.dot_general(
        left,
        right,
        (((left_dim,), (right_dim,)), ((), ())),
        preferred_element_type=jnp.float32,
    )


def rotate(x, axis, shift, stride=1):
    size = lax.axis_size(axis)
    return lax.ppermute(
        x, axis, [(src, (src + shift * stride) % size) for src in range(size)]
    )


def swap_core(x):
    size = lax.axis_size("gz")
    return lax.ppermute(x, "gz", [(src, src ^ 1) for src in range(size)])


def gather_rows(rows):
    nx, ny = lax.axis_size("gx"), lax.axis_size("gy")
    column = jnp.concatenate(
        [rows] + [rotate(rows, "gy", r) for r in range(1, ny)], axis=0
    )
    return jnp.concatenate(
        [column] + [rotate(column, "gx", s) for s in range(1, nx)], axis=0
    )


def scatter_rows(partial):
    nx, ny = lax.axis_size("gx"), lax.axis_size("gy")
    own, *others = jnp.split(partial, nx, axis=0)
    for s, block in enumerate(others, 1):
        own = own + rotate(block.astype(jnp.bfloat16), "gx", -s).astype(jnp.float32)
    own, *others = jnp.split(own, ny, axis=0)
    for r, block in enumerate(others, 1):
        own = own + rotate(block.astype(jnp.bfloat16), "gy", -r).astype(jnp.float32)
    return own.astype(jnp.bfloat16)


def half(rows, which):
    count = rows.shape[0] // 2
    return lax.dynamic_slice_in_dim(rows, which * count, count, 0)


def summed_half(rows, weights, weight_dim, core):
    away = contract(half(rows, 1 - core), weights, 1, weight_dim)
    near = swap_core(away.astype(jnp.bfloat16))
    total = contract(half(rows, core), weights, 1, weight_dim)
    total = total + near.astype(jnp.float32)
    mine = total.astype(jnp.bfloat16)
    for s in range(1, lax.axis_size("gz") // 2):
        total = total + rotate(mine, "gz", s, 2).astype(jnp.float32)
    return total


def both_halves(mine, core):
    other = swap_core(mine)
    first = jnp.where(core == 0, mine, other)
    second = jnp.where(core == 0, other, mine)
    return jnp.concatenate([first, second], axis=0)


def per_device(tokens, grad_out, w_in, w_out):
    nx, ny = lax.axis_size("gx"), lax.axis_size("gy")
    core = lax.axis_index("gz") % 2
    block_scale = 1.0 / math.sqrt(tokens.shape[0] * ny)
    tok_rows = gather_rows(tokens)
    grad_rows = gather_rows(grad_out)
    pre = summed_half(tok_rows, w_in, 0, core)
    act, slope = gelu_and_slope(pre)
    act_all = both_halves(act.astype(jnp.bfloat16), core)
    mlp_out = scatter_rows(contract(act_all, w_out, 1, 0))
    d_act = summed_half(grad_rows, w_out, 1, core)
    d_pre = both_halves((d_act * slope).astype(jnp.bfloat16), core)
    tok_grad = scatter_rows(contract(d_pre, w_in, 1, 1))
    wout_grad = contract(act_all, grad_rows, 0, 0) * block_scale
    win_grad = contract(tok_rows, d_pre, 0, 0) * block_scale
    return (mlp_out, tok_grad, win_grad, wout_grad)


def solution(mesh):
    in_specs = (
        P(("gx", "gy"), "gz"),
        P(("gx", "gy"), "gz"),
        P("gz", ("gy", "gx")),
        P(("gy", "gx"), "gz"),
    )
    out_specs = (
        P(("gx", "gy"), "gz"),
        P(("gx", "gy"), "gz"),
        P("gz", ("gy", "gx")),
        P(("gy", "gx"), "gz"),
    )
    return jax.shard_map(
        per_device, mesh=mesh, in_specs=in_specs, out_specs=out_specs, check_vma=False
    )
```
